256 devices in a mesh: gx: 8 (over x, core), gy: 4 (over y), gz: 8 (over z).
Axes of the slice: x: 4, y: 4, z: 8, core: 2. Of those that a mesh axis runs over, the one named last changes fastest.
Arguments:
- query: bfloat16 [4, 4, 4096], replicated, may hold values from -50 to 50
- keys: bfloat16 [32768, 4, 4096], P(('gx', 'gy', 'gz')), may hold values from -6 to 6
- values: bfloat16 [32768, 4, 4096], P(('gx', 'gy', 'gz')), may hold values from -6 to 6
- lm_keys: bfloat16 [1024, 4, 4096], P(('gx', 'gy', 'gz')), may hold values from -10 to 10
- lm_values: bfloat16 [1024, 4, 4096], P(('gx', 'gy', 'gz')), may hold values from -6 to 6
- selected: int32 [4, 16, 16], replicated, may hold values from 0 to 1023, as said below
Outputs:
- attended: float32 [4, 4, 4096], P(None, None, ('gx', 'gy', 'gz'))
The draws below stay inside these ranges and needn't reach their ends.
Inputs may be any that keep to these rules, and one draw needn't show every extreme that they name: `selected`: each batch row and head names 16 different blocks; every shard holds either none of them or exactly 2.
All inputs are finite; a program needn't handle non-finite values.
Results may differ from the reference program's by a relative error of at most 0.0007.
Values sent between devices are 32-bit elements; how exact they have to be, the bound alone decides.
No kernel may reach another device: no remote copies, remote signals or barrier semaphores. Data moves between devices by JAX's collectives and lax.ppermute only.
A program may use at most 64 MiB of HBM per device.

```python
import math
import jax
import jax.numpy as jnp
from jax import lax

H = 16
HD = 256
B = 4
QPOS = 4
TOK_DEV = 128
BLK = 32
TOPB = 16
CAP = 2
TOKENS = 32768
NBLK = 1024
N_GX = 8
N_GY = 4
N_GZ = 8


def pick_blocks(key):
    local_blocks = TOK_DEV // BLK
    device_count = NBLK // local_blocks
    group_count = TOPB // CAP
    first_key = jax.random.fold_in(key, 101)
    second_key = jax.random.fold_in(key, 103)
    raw_score = jax.random.randint(first_key, (B * H, device_count), 0, device_count)
    ladder = jnp.arange(device_count, dtype=jnp.int32)
    ranking = (raw_score + ladder) * device_count + ladder
    unused_values, owners = lax.top_k(ranking, group_count)
    random_rank = jax.random.randint(second_key, (B * H, group_count, local_blocks), 0, 1 << 20)
    ranked = random_rank * local_blocks + jnp.arange(local_blocks, dtype=jnp.int32)
    inner = jnp.argsort(ranked, axis=-1)[:, :, :CAP].astype(jnp.int32)
    return (owners[:, :, None].astype(jnp.int32) * local_blocks + inner).reshape(B, H, TOPB).astype(jnp.int32)


def cache_keys(key):
    draw_key = jax.random.fold_in(key, 211)
    field = jnp.clip(jax.random.normal(draw_key, (TOKENS, B, H * HD), jnp.float32), -6.0, 6.0)
    return field


def draw_keys(key, part):
    return cache_keys(key).astype(jnp.bfloat16)


def draw_selected(key, part):
    return pick_blocks(key)


def draw_query(key, part):
    draw_key = jax.random.fold_in(key, 307)
    field = jnp.clip(1.5 * jax.random.normal(draw_key, (B, QPOS, H * HD), jnp.float32), -9.0, 9.0)
    return field.astype(jnp.bfloat16)


def level_of(rng, dims, pieces, least, largest):
    def one(position, blocks):
        steps = jax.random.uniform(jax.random.fold_in(jax.random.fold_in(rng, 6), position), (blocks,), jnp.float32, least / len(pieces), largest / len(pieces))
        return jnp.repeat(jnp.exp(steps), dims[position] // blocks).reshape((-1,) + (1,) * (len(dims) - position - 1))

    factor_of = one(*pieces[0])
    for cut in pieces[1:]:
        factor_of = factor_of * one(*cut)
    return factor_of


def normal_values(rng, extent, scale, most, pieces=(), held_as=jnp.bfloat16):
    level = level_of(rng, extent, pieces, -0.22, 0.18) if pieces else 1.0
    entries = jax.random.normal(rng, extent, jnp.float32) * scale * level
    return jnp.minimum(jnp.maximum(entries, -most), most).astype(held_as)


def setup_inputs(seed: int = 0) -> dict:
    key_of = jax.random.split(jax.random.key(seed), 7)
    return {
        "query": draw_query(jax.random.fold_in(key_of[6], 71), 0),
        "keys": draw_keys(jax.random.fold_in(key_of[6], 71), 0),
        "values": normal_values(key_of[2], (TOKENS, B, H * HD), 1.0, 6.0, ((0, 256),)),
        "lm_keys": normal_values(key_of[3], (NBLK, B, H * HD), 1.7, 10.0, ((0, 256),)),
        "lm_values": normal_values(key_of[4], (NBLK, B, H * HD), 1.0, 6.0, ((0, 256),)),
        "selected": draw_selected(jax.random.fold_in(key_of[6], 71), 0),
    }


def reference(query, keys, values, lm_keys, lm_values, selected):
    shard_count = N_GX * N_GY * N_GZ
    local_blocks = TOK_DEV // BLK
    query_heads = query.reshape(B, QPOS, H, HD).astype(jnp.float32)
    score_scale = 1.0 / math.sqrt(HD)

    def shard_terms(shard):
        keys_here = lax.dynamic_slice_in_dim(keys, shard * TOK_DEV, TOK_DEV, 0).reshape(TOK_DEV, B, H, HD).astype(jnp.float32)
        values_here = lax.dynamic_slice_in_dim(values, shard * TOK_DEV, TOK_DEV, 0).reshape(TOK_DEV, B, H, HD).astype(jnp.float32)
        summary_keys = lax.dynamic_slice_in_dim(lm_keys, shard * local_blocks, local_blocks, 0).reshape(local_blocks, B, H, HD).astype(jnp.float32)
        summary_values = lax.dynamic_slice_in_dim(lm_values, shard * local_blocks, local_blocks, 0).reshape(local_blocks, B, H, HD).astype(jnp.float32)
        block_ids = shard * local_blocks + jnp.arange(local_blocks, dtype=jnp.int32)
        chosen_here = jnp.any(selected[:, :, :, None] == block_ids[None, None, None, :], axis=2)
        live_tokens = jnp.repeat(chosen_here, BLK, axis=2)
        token_score = jnp.einsum('bphd,tbhd->bpht', query_heads, keys_here) * score_scale
        token_score = jnp.where(live_tokens[:, None], token_score, -jnp.inf)
        summary_score = jnp.einsum('bphd,lbhd->bphl', query_heads, summary_keys) * score_scale
        local_peak = jnp.maximum(lax.optimization_barrier(jnp.max(token_score, -1)), lax.optimization_barrier(jnp.max(summary_score, -1)))
        token_weight = jnp.exp(token_score - local_peak[..., None])
        summary_weight = jnp.exp(summary_score - local_peak[..., None])
        local_total = lax.optimization_barrier(jnp.sum(token_weight, -1)) + lax.optimization_barrier(jnp.sum(summary_weight, -1))
        token_round = lax.optimization_barrier(token_weight.astype(jnp.bfloat16)).astype(jnp.float32)
        summary_round = lax.optimization_barrier(summary_weight.astype(jnp.bfloat16)).astype(jnp.float32)
        local_sum = jnp.einsum('bpht,tbhd->bphd', token_round, values_here) + jnp.einsum('bphl,lbhd->bphd', summary_round, summary_values)
        return (local_peak, local_total, local_sum)
    peaks, totals, sums = lax.map(shard_terms, jnp.arange(shard_count, dtype=jnp.int32))
    global_peak = lax.optimization_barrier(jnp.max(peaks, 0))
    rescale = jnp.exp(peaks - global_peak[None])
    numerator = lax.optimization_barrier(jnp.sum(rescale[..., None] * sums, 0))
    denominator = lax.optimization_barrier(jnp.sum(rescale * totals, 0))
    return (numerator / denominator[..., None]).reshape(B, QPOS, H * HD)
```

```python
import math

import jax
import jax.numpy as jnp
from jax import lax
from jax.experimental import pallas as pl
from jax.experimental.pallas import tpu as pltpu
from jax.sharding import Mesh
from jax.sharding import PartitionSpec as P

AXES = ("x", "core", "gy", "gz")
CHIP_AXES = ("x", "gy", "gz")
HEADS = 16
LANES = 128
NEG_INF = float("-inf")


def attend_kernel(
    query_ref, selected_ref, summary_key_ref, summary_value_ref, keys_hbm, values_hbm,
    keep_ref, send_ref, key_buf, value_buf, rows_ref, key_sems, value_sems,
):
    my_core = lax.axis_index("core")
    my_index = lax.axis_index(AXES)

    def head_of(slot):
        half, pos = slot // 8, slot % 8
        core = my_core if half == 0 else 1 - my_core
        return (pos // 2) * 4 + core * 2 + pos % 2

    order = [8 + i for i in range(8)] + list(range(8))

    def copies(hbm, buf, sems, slot):
        head = head_of(slot)
        return [
            pltpu.make_async_copy(hbm.at[:, 2 * head + i], buf.at[slot, i], sems.at[slot, i]) for i in range(2)
        ]

    for slot in order:
        for cp in copies(keys_hbm, key_buf, key_sems, slot):
            cp.start()
        for cp in copies(values_hbm, value_buf, value_sems, slot):
            cp.start()

    row = lax.broadcasted_iota(jnp.int32, (16, LANES), 0) // 4
    lane = lax.broadcasted_iota(jnp.int32, (16, LANES), 1)
    same_row = row == lane % 4
    same_row16 = same_row[:, :16]
    scale = 1.0 / math.sqrt(2 * LANES)
    nt = (((1,), (1,)), ((), ()))
    nn = (((1,), (0,)), ((), ()))

    def small(ref, head):
        parts = [ref[:, 2 * head + i].reshape(16, LANES) for i in range(2)]
        return jnp.concatenate(parts, axis=1)

    def big(buf, slot):
        parts = [buf.at[slot, i].reshape(512, LANES)[...] for i in range(2)]
        return jnp.concatenate(parts, axis=1)

    def scores(slot):
        head = head_of(slot)
        for cp in copies(keys_hbm, key_buf, key_sems, slot):
            cp.wait()
        q = small(query_ref, head)
        s = lax.dot_general(q, big(key_buf, slot), nt, preferred_element_type=jnp.float32) * scale
        s2 = lax.dot_general(q, small(summary_key_ref, head), nt, preferred_element_type=jnp.float32) * scale
        chosen = selected_ref[head]
        tiles = []
        for blk in range(4):
            here = jnp.max(jnp.where(chosen == my_index * 4 + blk, 1.0, 0.0), axis=1, keepdims=True)
            ok = same_row & (here > 0.0)
            tiles.append(jnp.where(ok, s[:, blk * LANES:(blk + 1) * LANES], NEG_INF))
        return tiles, jnp.where(same_row16, s2, NEG_INF)

    def weights(tiles, s2):
        top = jnp.maximum(jnp.maximum(tiles[0], tiles[1]), jnp.maximum(tiles[2], tiles[3]))
        peak = jnp.maximum(jnp.max(top, axis=1, keepdims=True), jnp.max(s2, axis=1, keepdims=True))
        w = [jnp.exp(t - peak) for t in tiles]
        w2 = jnp.exp(s2 - peak)
        total = jnp.sum(w[0] + w[1] + (w[2] + w[3]), axis=1, keepdims=True) + jnp.sum(w2, axis=1, keepdims=True)
        return jnp.concatenate([t.astype(jnp.bfloat16) for t in w], axis=1), w2.astype(jnp.bfloat16), peak, total

    def weighted(slot, w, w2, peak, total):
        for cp in copies(values_hbm, value_buf, value_sems, slot):
            cp.wait()
        out = lax.dot_general(w, big(value_buf, slot), nn, preferred_element_type=jnp.float32)
        out = out + lax.dot_general(
            w2, small(summary_value_ref, head_of(slot)), nn, preferred_element_type=jnp.float32
        )
        half, pos = slot // 8, slot % 8
        for bp in range(16):
            rows_ref[half, 0, bp, pos:pos + 1, :] = out[bp:bp + 1, :LANES]
            rows_ref[half, 1, bp, pos:pos + 1, :] = out[bp:bp + 1, LANES:]
            rows_ref[half, 2, bp, pos:pos + 1, :] = jnp.broadcast_to(peak[bp:bp + 1], (1, LANES))
            rows_ref[half, 3, bp, pos:pos + 1, :] = jnp.broadcast_to(total[bp:bp + 1], (1, LANES))

    stage_a, stage_b = {}, {}
    for step in range(len(order) + 2):
        if step < len(order):
            stage_a[step] = scores(order[step])
        if 0 <= step - 1 < len(order):
            stage_b[step - 1] = weights(*stage_a.pop(step - 1))
        if 0 <= step - 2 < len(order):
            weighted(order[step - 2], *stage_b.pop(step - 2))

    lane8 = lax.broadcasted_iota(jnp.int32, (8, LANES), 1)
    for half, out_ref in ((0, keep_ref), (1, send_ref)):
        for hi in range(2):
            for tile in range(2):
                a = [rows_ref[half, tile, hi * 8 + i] for i in range(8)]
                for bit in range(3):
                    step = 1 << bit
                    width = 16 * step
                    upper = (lane8 // width) % 2 == 1
                    for i in range(8):
                        if i & step:
                            continue
                        u, v = a[i], a[i | step]
                        a[i] = jnp.where(upper, pltpu.roll(v, width, 1), u)
                        a[i | step] = jnp.where(upper, v, pltpu.roll(u, LANES - width, 1))
                for i in range(8):
                    out_ref[pl.ds((tile * 8 + i) * 3 + hi, 8, stride=48), :] = a[i]
        group, part = lane8 // 16, (lane8 % 16) // 4
        extra = jnp.zeros((8, LANES), jnp.float32)
        for what in range(4):
            for i in range(8):
                value = rows_ref[half, 2 + what // 2, (what % 2) * 8 + i]
                extra = jnp.where((group == i) & (part == what), value, extra)
        for d in range(16):
            out_ref[pl.ds(d * 3 + 2, 8, stride=48), :] = extra


def spread(x, lane, offset):
    if offset:
        x = jnp.where(lane % 8 < 4, pltpu.roll(x, LANES - 4, 1), x)
    else:
        x = jnp.where(lane % 8 < 4, x, pltpu.roll(x, 4, 1))
    return jnp.where(lane % 16 < 8, x, pltpu.roll(x, 8, 1))


def pair_kernel(first_ref, second_ref, out_ref):
    n = first_ref.shape[0] // 3
    lane = lax.broadcasted_iota(jnp.int32, (n, LANES), 1)
    e = [r[pl.ds(2, n, stride=3), :] for r in (first_ref, second_ref)]
    peak = jnp.maximum(e[0], e[1])
    f = [jnp.exp(t - peak) for t in e]
    total = sum(ft * pltpu.roll(t, LANES - 8, 1) for ft, t in zip(f, e))
    out_ref[pl.ds(2, n, stride=3), :] = jnp.where(lane % 16 < 8, peak, pltpu.roll(total, 8, 1))
    for hi in range(2):
        g = [spread(t, lane, 4 * hi) for t in f]
        out_ref[pl.ds(hi, n, stride=3), :] = (
            first_ref[pl.ds(hi, n, stride=3), :] * g[0] + second_ref[pl.ds(hi, n, stride=3), :] * g[1]
        )


def merge_kernel(parts_ref, out_ref):
    n = parts_ref.shape[0] // 3
    lane = lax.broadcasted_iota(jnp.int32, (n, LANES), 1)
    e = parts_ref[pl.ds(2, n, stride=3), :]
    f = jnp.exp(e - jnp.max(e, axis=0, keepdims=True))
    total = jnp.sum(f * pltpu.roll(e, LANES - 8, 1), axis=0, keepdims=True)
    for hi in range(2):
        g = spread(f, lane, 4 * hi)
        num = jnp.sum(parts_ref[pl.ds(hi, n, stride=3), :] * g, axis=0, keepdims=True)
        den = spread(jnp.broadcast_to(total, (8, LANES)), lane[:8], 4 * hi)
        res = jnp.broadcast_to(num, (8, LANES)) / den
        for i in range(8):
            row = hi * 8 + i
            out_ref[row // 4, row % 4:row % 4 + 1, :] = pltpu.roll(res, LANES - 16 * i, 1)[:1, :16] if i else res[:1, :16]


def body(query, keys, values, lm_keys, lm_values, selected):
    def tiled(a):
        lead, rows, width = a.shape
        return a.reshape(lead, rows, width // LANES, LANES).transpose(0, 2, 1, 3)

    vmem = pl.BlockSpec(memory_space=pltpu.VMEM)
    hbm = pl.BlockSpec(memory_space=pltpu.HBM)
    chosen = jnp.repeat(selected.transpose(1, 0, 2), query.shape[1], axis=1)
    state = jax.ShapeDtypeStruct((128 * 3, LANES), jnp.float32)
    keep, send = pl.pallas_call(
        attend_kernel,
        out_shape=(state, state),
        in_specs=[vmem, vmem, vmem, vmem, hbm, hbm],
        out_specs=(vmem, vmem),
        scratch_shapes=[
            pltpu.VMEM((HEADS, 2, 128, 4, LANES), jnp.bfloat16),
            pltpu.VMEM((HEADS, 2, 128, 4, LANES), jnp.bfloat16),
            pltpu.VMEM((2, 4, 16, 8, LANES), jnp.float32),
            pltpu.SemaphoreType.DMA((HEADS, 2)),
            pltpu.SemaphoreType.DMA((HEADS, 2)),
        ],
        compiler_params=pltpu.CompilerParams(vmem_limit_bytes=61 * 1024 * 1024),
        name="attend",
    )(tiled(query), chosen, tiled(lm_keys), tiled(lm_values), tiled(keys), tiled(values))
    other = lax.ppermute(send, "core", [(0, 1), (1, 0)])
    both = pl.pallas_call(
        pair_kernel, out_shape=state, in_specs=[vmem, vmem], out_specs=vmem, name="pair",
        compiler_params=pltpu.CompilerParams(vmem_limit_bytes=4 * 1024 * 1024),
    )(keep, other)
    parts = lax.all_to_all(both.reshape(128, 1, 3 * LANES), CHIP_AXES, 0, 0, tiled=True)
    return pl.pallas_call(
        merge_kernel,
        out_shape=jax.ShapeDtypeStruct((4, 4, 16), jnp.float32),
        in_specs=[vmem],
        out_specs=vmem,
        name="merge",
        compiler_params=pltpu.CompilerParams(vmem_limit_bytes=4 * 1024 * 1024),
    )(parts.reshape(128 * 3, LANES))


def solution(mesh):
    torus = Mesh(mesh.devices.reshape(4, 2, mesh.shape["gy"], mesh.shape["gz"]), AXES)
    split = P(AXES, None, None)
    return jax.shard_map(
        body,
        mesh=torus,
        in_specs=(P(), split, split, split, split, P()),
        out_specs=P(None, None, AXES),
        check_vma=False,
    )
```
